256 devices in a mesh: dp: 16 (over x, y_lo, core), seq: 16 (over y_hi, z).
Axes of the slice: x: 4, y: 4 (y_hi: 2, y_lo: 2; y = y_hi * 2 + y_lo), z: 8, core: 2. Of those that a mesh axis runs over, the one named last changes fastest.
Arguments:
- query: bfloat16 [16, 2048, 2048], P('dp', 'seq'), may hold values from -8 to 8
- key_value: bfloat16 [2, 16, 2048, 2048], P(None, 'dp', 'seq'), may hold values from -8 to 8
- grad_y: bfloat16 [16, 2048, 2048], P('dp', 'seq'), may hold values from -6 to 6
- tags: int32 [16, 2048], P('dp', 'seq'), may hold values 0 or 1
- segments: int32 [16, 2048], P('dp'), may hold values from 0 to 15, never falling along the last dimension, each value on 1 to 256 neighbouring positions
- out_weight: bfloat16 [2, 2048, 2048], P(None, None, 'dp'), may hold values from -0.125 to 0.125
Outputs:
- grad_query: bfloat16 [16, 2048, 2048], P('dp', 'seq')
- grad_key_value: bfloat16 [2, 16, 2048, 2048], P(None, 'dp', 'seq')
The draws below stay inside these ranges and needn't reach their ends.
Inputs may be any that keep to these rules, and one draw needn't show every extreme that they name: `segments`: sample numbers never fall along a sequence; a sample holds at most 256 positions and some sample holds exactly 256.
All inputs are finite; a program needn't handle non-finite values. No bound on the sum of `tags` on one device may be relied on, other than what follows from the above.
Results may differ from the reference program's by a relative error of at most 0.0075.
Values may be sent and summed in bfloat16 or wider, within the bound.
A program may use at most 128 MiB of HBM per device.

```python
import math
import jax
import jax.numpy as jnp
import numpy as np
from jax import lax

HEADS = 16
HEAD_DIM = 128
DW = 2048
REACH = 2
T_DEV = 128
HC = 2048
LENGTH = 2048
SEQS = 16
SAMPLES = 16


def draw_query(key, part):
    base = jnp.clip(jax.random.normal(jax.random.fold_in(key, 1), (SEQS, LENGTH, HC), jnp.float32), -6.0, 6.0)
    return base.astype(jnp.bfloat16)


def draw_key_value(key, part):
    base = jnp.clip(jax.random.normal(jax.random.fold_in(key, 2), (2, SEQS, LENGTH, HC), jnp.float32), -6.0, 6.0)
    return base.astype(jnp.bfloat16)


def set_ends(entries, own_key, smallest, largest):
    longest = entries.shape.index(max(entries.shape))
    spots = []
    for shift in (0, 1):
        where = [jax.random.randint(jax.random.fold_in(own_key, axis), (), 0, length) for axis, length in enumerate(entries.shape)]
        where[longest] = (where[longest] + shift) % entries.shape[longest]
        spots.append(tuple(where))
    return entries.at[spots[0]].set(smallest).at[spots[1]].set(largest)


def levels(stream_key, dims, cuts, least, largest):
    loudness = 1.0
    for dim, parts in cuts:
        steps = jax.random.uniform(jax.random.fold_in(jax.random.fold_in(stream_key, 6), dim), (parts,), jnp.float32, least / len(cuts), largest / len(cuts))
        loudness = loudness * jnp.repeat(jnp.exp(steps), dims[dim] // parts).reshape((-1,) + (1,) * (len(dims) - 1 - dim))
    return loudness


def profile(number_of, total, reach, lean):
    loads = [(1 << 20) // math.isqrt(standing ** lean) + 1 for standing in range(2, number_of + 1)]
    surplus, holding = total - reach - (number_of - 1), [1] * (number_of - 1)
    while surplus > 0:
        movable = [i for i in range(number_of - 1) if holding[i] < reach]
        pool, remaining = sum([loads[i] for i in movable]), surplus
        for i in movable:
            addition = min(reach - holding[i], max(1, remaining * loads[i] // pool), surplus)
            holding[i] = holding[i] + addition
            surplus = surplus - addition
    return np.array([reach] + holding)


def uneven(stream_key, amount, total, bound, skew):
    if amount == 2:
        one = jax.random.randint(stream_key, (), max(1, total - bound), min(bound, total - 1) + 1)
        return jnp.stack([one, total - one])
    tallies = jnp.asarray(profile(amount, total, bound, skew), jnp.int32)
    twos = (amount - 1) // 2
    donor, receiver = tallies[1:1 + 2 * twos:2], tallies[2:2 + 2 * twos:2]
    margin = jnp.minimum(donor - 1, bound - receiver)
    shifted = jax.random.randint(jax.random.fold_in(stream_key, 1), (twos,), 0, 1 << 20) % (margin + 1)
    tallies = tallies.at[1:1 + 2 * twos:2].set(donor - shifted).at[2:2 + 2 * twos:2].set(receiver + shifted)
    return tallies[jax.random.permutation(jax.random.fold_in(stream_key, 2), amount)]


def scatter_about(rng, shape, deviation, most, cuts=(), kind=jnp.bfloat16):
    values = jax.random.normal(rng, shape, jnp.float32) * deviation
    if len(cuts) > 0:
        values = levels(rng, shape, cuts, -0.22, 0.18) * values
    return jnp.clip(values, min=-most, max=most).astype(kind)


def setup_inputs(seed: int = 0) -> dict:
    seeds = jax.random.split(jax.random.key(seed), 7)
    return {
        "query": draw_query(jax.random.fold_in(seeds[6], 71), 0),
        "key_value": draw_key_value(jax.random.fold_in(seeds[6], 71), 0),
        "grad_y": scatter_about(seeds[2], (SEQS, LENGTH, DW), 1.0, 6.0, ((0, 16), (1, 16))),
        "tags": set_ends((jax.random.randint(seeds[3], (SEQS, LENGTH), 0, 2) < 1).astype(jnp.int32), jax.random.fold_in(seeds[3], 1), 0, 1),
        "segments": jax.vmap(lambda own: jnp.searchsorted(jnp.cumsum(uneven(own, SAMPLES, LENGTH, REACH * T_DEV, 0)), jnp.arange(LENGTH), side="right"))(jax.random.split(seeds[4], SEQS)).reshape((SEQS, LENGTH)).astype(jnp.int32),
        "out_weight": scatter_about(seeds[5], (2, HC, DW), DW ** -0.5, 0.125, ((2, 16),)),
    }


NEG = -1e30


def block_grads(query, keys, values, grad_out, mask):
    scale = HEAD_DIM ** -0.5
    qf = query.astype(jnp.float32)
    kf = keys.astype(jnp.float32)
    vf = values.astype(jnp.float32)
    gf = grad_out.astype(jnp.float32)
    scores = jnp.einsum("qhe,khe->hqk", qf, kf) * scale
    scores = jnp.where(mask[None], scores, NEG)
    top = jnp.max(scores, axis=2, keepdims=True)
    lse = top + jnp.log(jnp.sum(jnp.exp(scores - top), axis=2, keepdims=True))
    probs = jnp.exp(scores - lse)
    probs_low = lax.optimization_barrier(probs.astype(jnp.bfloat16)).astype(jnp.float32)
    dprob = jnp.einsum("qhe,khe->hqk", gf, vf)
    delta = jnp.sum(probs * dprob, axis=2, keepdims=True)
    dscore = lax.optimization_barrier((probs * (dprob - delta) * scale).astype(jnp.bfloat16)).astype(jnp.float32)
    grad_q = jnp.einsum("hqk,khe->qhe", dscore, kf)
    grad_k = jnp.einsum("hqk,qhe->khe", dscore, qf)
    grad_v = jnp.einsum("hqk,qhe->khe", probs_low, gf)
    return grad_q, grad_k, grad_v


def one_sequence(query, keys, values, grad, tags, segs, out_weight):
    text_part = jnp.dot(grad, out_weight[1].T, preferred_element_type=jnp.float32)
    image_part = jnp.dot(grad, out_weight[0].T, preferred_element_type=jnp.float32)
    grad_out = jnp.where(tags[:, None] == 1, text_part, image_part).astype(jnp.bfloat16)
    count = LENGTH // T_DEV

    def split(array):
        return array.reshape((count, T_DEV, HEADS, HEAD_DIM))

    def padded(array):
        return jnp.concatenate([jnp.zeros((REACH,) + array.shape[1:], array.dtype), array], axis=0)

    query_b = split(query)
    key_pad = padded(split(keys))
    value_pad = padded(split(values))
    grad_b = split(grad_out)
    seg_b = segs.reshape((count, T_DEV))
    seg_pad = jnp.concatenate([jnp.full((REACH, T_DEV), -1, seg_b.dtype), seg_b], axis=0)
    width = (REACH + 1) * T_DEV

    def one_block(number):
        k_win = lax.dynamic_slice_in_dim(key_pad, number, REACH + 1, 0).reshape((width, HEADS, HEAD_DIM))
        v_win = lax.dynamic_slice_in_dim(value_pad, number, REACH + 1, 0).reshape((width, HEADS, HEAD_DIM))
        s_win = lax.dynamic_slice_in_dim(seg_pad, number, REACH + 1, 0).reshape((width,))
        q_blk = query_b[number]
        g_blk = grad_b[number]
        s_blk = seg_b[number]
        q_pos = number * T_DEV + jnp.arange(T_DEV).astype(jnp.int32)
        k_pos = (number - REACH) * T_DEV + jnp.arange(width).astype(jnp.int32)
        mask = (s_blk[:, None] == s_win[None, :]) & (k_pos[None, :] <= q_pos[:, None])
        return block_grads(q_blk, k_win, v_win, g_blk, mask)

    grad_q, grad_k, grad_v = lax.map(one_block, jnp.arange(count).astype(jnp.int32))

    def fold(array):
        total = jnp.zeros((count + REACH, T_DEV, HEADS, HEAD_DIM), jnp.float32)
        for offset in range(REACH + 1):
            part = array[:, offset * T_DEV:(offset + 1) * T_DEV]
            total = total + jnp.pad(part, ((offset, REACH - offset), (0, 0), (0, 0), (0, 0)))
        return total[REACH:].reshape((LENGTH, HC)).astype(jnp.bfloat16)

    return grad_q.reshape((LENGTH, HC)).astype(jnp.bfloat16), fold(grad_k), fold(grad_v)


def reference(query, key_value, grad_y, tags, segments, out_weight):
    def per_sequence(number):
        return one_sequence(query[number], key_value[0, number], key_value[1, number], grad_y[number], tags[number], segments[number], out_weight)

    grad_q, grad_k, grad_v = lax.map(per_sequence, jnp.arange(SEQS).astype(jnp.int32))
    return grad_q, jnp.stack([grad_k, grad_v])
```

```python
import jax
import jax.numpy as jnp
from jax import lax
from jax.experimental import pallas as pl
from jax.experimental.pallas import tpu as pltpu
from jax.sharding import PartitionSpec as P

HEAD_DIM = 128
ROWS = 128
WIDTH = 2048
REACH = 2
PART = 512
CHUNK = 256
COUNT = WIDTH // CHUNK
SCALE = HEAD_DIM ** -0.5
NEG = -1e30
F32 = jnp.float32
BF16 = jnp.bfloat16
MESH = pl.DeviceIdType.MESH
LAST = (((1,), (1,)), ((), ()))
FIRST = (((0,), (0,)), ((), ()))


def down(row):
    return jnp.broadcast_to(row.astype(F32), (ROWS, ROWS)).T


def kernel(
    q_ref, kv_ref, gy_ref, tags_ref, seg_ref, w_ref, gq_ref, gkv_ref,
    wg, gyb, tagb, gm, psend, precv, pown, near, far, bias, t1, t0, sa, ra, sb, rb,
    w_sem, s_gy, r_gy, s_tag, r_tag, s_w, r_w, s_p, r_p, s_kv, r_kv,
):
    dp, seq = lax.axis_index("dp"), lax.axis_index("seq")
    x, slot, core = lax.div(dp, 4), lax.rem(dp, 4), lax.rem(dp, 2)
    y_lo = lax.div(slot, 2)
    other = lax.rem(slot + 2, 4)
    after, before = (dp, lax.rem(seq + 1, 16)), (dp, lax.rem(seq + 15, 16))
    beside = dp + 2 - 4 * y_lo
    above = (beside, lax.rem(seq + 8 * y_lo, 16))
    below = (beside, lax.rem(seq + 8 - 8 * y_lo, 16))
    partner = (dp + 1 - 2 * core, seq)
    across = [None] + [(lax.rem(dp + 4 * o, 16), seq) for o in range(1, 4)]

    load = pltpu.make_async_copy(
        w_ref, wg.at[:, :, pl.ds(pl.multiple_of(slot * 128, 128), 128)], w_sem
    )
    load.start()
    barrier = pltpu.get_barrier_semaphore()
    for peer in (after, before, above, below, partner, *across[1:]):
        pl.semaphore_signal(barrier, inc=1, device_id=peer, device_id_type=MESH)
    pl.semaphore_wait(barrier, 8)

    def remote(src, dst, send, recv, to):
        return pltpu.make_async_remote_copy(
            src_ref=src, dst_ref=dst, send_sem=send, recv_sem=recv,
            device_id=to, device_id_type=MESH,
        )

    def cols(c):
        return pl.ds(pl.multiple_of(c * CHUNK, CHUNK), CHUNK)

    def place(number):
        return pl.ds(pl.multiple_of(number * 128, 128), 128)

    def tags_to(o):
        return remote(tags_ref, tagb.at[3 - o], s_tag.at[o - 1], r_tag.at[3 - o], across[o])

    def grad_to(o):
        part = pl.ds(pl.multiple_of(lax.rem(x + o, 4) * PART, PART), PART)
        return remote(gy_ref.at[:, part], gyb.at[3 - o], s_gy.at[o - 1], r_gy.at[3 - o], across[o])

    def weight_to(kind, c):
        piece = wg.at[:, cols(c), place(slot)]
        if kind == 0:
            piece, to = wg.at[0, cols(c), place(slot)], above
        elif kind == 1:
            piece, to = wg.at[1, cols(c), place(slot)], below
        elif kind == 2:
            to = partner
        else:
            piece, to = wg.at[:, cols(c), place(other)], partner
        return remote(piece, piece, s_w.at[kind, c], r_w.at[kind, c], to)

    def partial_to(o, c):
        return remote(
            psend.at[o - 1, :, cols(c)], precv.at[3 - o, :, cols(c)],
            s_p.at[o - 1, c], r_p.at[3 - o, c], across[o],
        )

    def kv_to(kind, c):
        src, dst, to = (
            (kv_ref, near, after), (near, far, after), (sa, ra, before), (sb, rb, before)
        )[kind]
        return remote(
            src.at[:, :, cols(c)], dst.at[:, :, cols(c)], s_kv.at[kind, c], r_kv.at[kind, c], to
        )

    for o in (2, 1, 3):
        tags_to(o).start()
        grad_to(o).start()
    kv_to(0, 0).start()
    kv_to(0, 1).start()
    load.wait()

    @pl.loop(0, COUNT)
    def _(c):
        for kind in (0, 1, 2):
            weight_to(kind, c).start()

    own_row = seg_ref[:, place(seq)]
    for back in range(REACH, -1, -1):
        key_row = seg_ref[:, place(jnp.maximum(seq - back, 0))]
        same = down(key_row) == jnp.broadcast_to(own_row.astype(F32), (ROWS, ROWS))
        if back == 0:
            key = lax.broadcasted_iota(jnp.int32, (ROWS, ROWS), 0)
            query = lax.broadcasted_iota(jnp.int32, (ROWS, ROWS), 1)
            block = jnp.where(jnp.logical_and(same, key <= query), 0.0, NEG)
        else:
            block = jnp.where(same, jnp.where(seq >= back, 0.0, NEG).astype(F32), NEG)
        bias[(REACH - back) * ROWS : (REACH - back + 1) * ROWS, :] = block

    for r in range(4):
        if r > 0:
            tags_to(4 - r).wait_recv()
            grad_to(4 - r).wait_recv()
            text = down(tagb[r - 1]) == 1.0
        else:
            text = down(tags_ref[...]) == 1.0
        for j in range(4):
            if r > 0:
                block = gyb[r - 1, :, j * 128 : (j + 1) * 128]
            else:
                block = gy_ref[:, place(x * 4 + j)]
            block = block.astype(F32)
            rows = slice(r * ROWS, (r + 1) * ROWS)
            gm[rows, j * 128 : (j + 1) * 128] = jnp.where(text, block, 0.0).astype(BF16)
            gm[rows, PART + j * 128 : PART + (j + 1) * 128] = jnp.where(text, 0.0, block).astype(BF16)

    def relay(c):
        weight_to(0, c).wait_recv()
        weight_to(1, c).wait_recv()
        weight_to(3, c).start()

    def project(c):
        weight_to(2, c).wait_recv()
        weight_to(3, c).wait_recv()
        total = lax.dot_general(
            gm[:, :PART], wg[1, cols(c), :], LAST, preferred_element_type=F32
        ) + lax.dot_general(gm[:, PART:], wg[0, cols(c), :], LAST, preferred_element_type=F32)
        pown[:, cols(c)] = total[:ROWS]
        for o in (2, 1, 3):
            psend[o - 1, :, cols(c)] = total[o * ROWS : (o + 1) * ROWS].astype(BF16)
            partial_to(o, c).start()

    def attend(c):
        for o in range(1, 4):
            partial_to(o, c).wait_recv()
        grad_out = pown[:, cols(c)]
        for r in range(3):
            grad_out = grad_out + precv[r, :, cols(c)].astype(F32)
        grad_out = grad_out.astype(BF16)
        kv_to(1, c).wait_recv()
        for h in range(CHUNK // HEAD_DIM):
            here = pl.ds(pl.multiple_of(c * CHUNK + h * HEAD_DIM, HEAD_DIM), HEAD_DIM)
            query = q_ref[:, here]
            grad = grad_out[:, h * HEAD_DIM : (h + 1) * HEAD_DIM]
            keys = jnp.concatenate([far[0, :, here], near[0, :, here], kv_ref[0, :, here]], axis=0)
            values = jnp.concatenate([far[1, :, here], near[1, :, here], kv_ref[1, :, here]], axis=0)
            scores = lax.dot_general(keys, query, LAST, preferred_element_type=F32)
            scores = scores * SCALE + bias[...]
            raised = jnp.exp(scores - jnp.max(scores, axis=0, keepdims=True))
            dprob = lax.dot_general(values, grad, LAST, preferred_element_type=F32)
            share = 1.0 / jnp.sum(raised, axis=0, keepdims=True)
            probs = raised * share
            delta = jnp.sum(probs * dprob, axis=0, keepdims=True)
            dscore = (probs * (dprob - delta) * SCALE).astype(BF16)
            grad_q = lax.dot_general(dscore, keys, FIRST, preferred_element_type=F32)
            gq_ref[:, here] = grad_q.astype(BF16)
            grad_k = jnp.dot(dscore, query, preferred_element_type=F32)
            grad_v = jnp.dot(probs.astype(BF16), grad, preferred_element_type=F32)
            for index, term in ((0, grad_k), (1, grad_v)):
                sa[index, :, here] = term[:ROWS].astype(BF16)
                t1[index, :, here] = term[ROWS : 2 * ROWS]
                t0[index, :, here] = term[2 * ROWS :]
        kv_to(2, c).start()

    def fold(c):
        kv_to(2, c).wait_recv()
        sb[:, :, cols(c)] = (ra[:, :, cols(c)].astype(F32) + t1[:, :, cols(c)]).astype(BF16)
        kv_to(3, c).start()

    def finish(c):
        kv_to(3, c).wait_recv()
        gkv_ref[:, :, cols(c)] = (rb[:, :, cols(c)].astype(F32) + t0[:, :, cols(c)]).astype(BF16)

    relay(0)
    relay(1)
    project(0)

    @pl.loop(0, COUNT + 3)
    def _(i):
        @pl.when(i < COUNT)
        def _():
            kv_to(0, i).wait_recv()
            kv_to(1, i).start()

        @pl.when(i + 2 < COUNT)
        def _():
            kv_to(0, i + 2).start()
            relay(i + 2)

        @pl.when(i + 1 < COUNT)
        def _():
            project(i + 1)

        @pl.when(jnp.logical_and(i >= 1, i <= COUNT))
        def _():
            attend(i - 1)

        @pl.when(jnp.logical_and(i >= 2, i <= COUNT + 1))
        def _():
            fold(i - 2)

        @pl.when(i >= 3)
        def _():
            finish(i - 3)

    for o in range(1, 4):
        tags_to(o).wait_send()
        grad_to(o).wait_send()

    @pl.loop(0, COUNT)
    def _(c):
        for kind in range(4):
            weight_to(kind, c).wait_send()
            kv_to(kind, c).wait_send()
        for o in range(1, 4):
            partial_to(o, c).wait_send()


def shards(query, key_value, grad_y, tags, segments, out_weight):
    vmem = pl.BlockSpec(memory_space=pltpu.VMEM)
    dma = pltpu.SemaphoreType.DMA
    pair = (2, ROWS, WIDTH)
    grad_q, grad_kv = pl.pallas_call(
        kernel,
        out_shape=(
            jax.ShapeDtypeStruct((ROWS, WIDTH), BF16),
            jax.ShapeDtypeStruct(pair, BF16),
        ),
        in_specs=[vmem] * 5 + [pl.BlockSpec(memory_space=pl.ANY)],
        out_specs=(vmem, vmem),
        scratch_shapes=[
            pltpu.VMEM((2, WIDTH, PART), BF16),
            pltpu.VMEM((3, ROWS, PART), BF16),
            pltpu.VMEM((3, 1, ROWS), jnp.int32),
            pltpu.VMEM((4 * ROWS, 2 * PART), BF16),
            pltpu.VMEM((3, ROWS, WIDTH), BF16),
            pltpu.VMEM((3, ROWS, WIDTH), BF16),
            pltpu.VMEM((ROWS, WIDTH), F32),
            pltpu.VMEM(pair, BF16),
            pltpu.VMEM(pair, BF16),
            pltpu.VMEM(((REACH + 1) * ROWS, ROWS), F32),
            pltpu.VMEM(pair, F32),
            pltpu.VMEM(pair, F32),
            pltpu.VMEM(pair, BF16),
            pltpu.VMEM(pair, BF16),
            pltpu.VMEM(pair, BF16),
            pltpu.VMEM(pair, BF16),
            dma,
            dma((3,)), dma((3,)), dma((3,)), dma((3,)),
            dma((4, COUNT)), dma((4, COUNT)),
            dma((3, COUNT)), dma((3, COUNT)),
            dma((4, COUNT)), dma((4, COUNT)),
        ],
        compiler_params=pltpu.CompilerParams(
            collective_id=1, has_side_effects=True, vmem_limit_bytes=48 << 20
        ),
        name="mixed_backward",
    )(query[0], key_value[:, 0], grad_y[0], tags, segments, out_weight)
    return grad_q[None], grad_kv[:, None]


def solution(mesh):
    return jax.shard_map(
        shards,
        mesh=mesh,
        in_specs=(
            P("dp", "seq", None),
            P(None, "dp", "seq", None),
            P("dp", "seq", None),
            P("dp", "seq"),
            P("dp", None),
            P(None, None, "dp"),
        ),
        out_specs=(P("dp", "seq", None), P(None, "dp", "seq", None)),
        check_vma=False,
    )
```

```python
import jax
import jax.numpy as jnp
from jax import lax
from jax.experimental import pallas as pl
from jax.experimental.pallas import tpu as pltpu
from jax.sharding import PartitionSpec as P

HEAD_DIM = 128
ROWS = 128
WIDTH = 2048
REACH = 2
PART = 512
CHUNK = 256
COUNT = WIDTH // CHUNK
HEADS = WIDTH // HEAD_DIM
LEAD = 4
BACK = 3
HOME = 3
SCALE = HEAD_DIM ** -0.5
NEG = -1e30
F32 = jnp.float32
BF16 = jnp.bfloat16
MESH = pl.DeviceIdType.MESH
LAST = (((1,), (1,)), ((), ()))
FIRST = (((0,), (0,)), ((), ()))


def down(row):
    return jnp.broadcast_to(row.astype(F32), (ROWS, ROWS)).T


def kernel(
    q_in, kv_in, gy_in, tags_in, seg_in, w_in, gq_ref, gkv_ref,
    q_ref, kv_ref, gy_ref, tags_ref, seg_ref, wg, gyb, tagb, gm, psend, precv, pown, near, far, bias, t1, t0, sa, ra, sb, rb,
    in_sem, kv_sem, s_gy, r_gy, s_tag, r_tag, s_w, r_w, s_p, r_p, s_kv, r_kv,
):
    dp, seq = lax.axis_index("dp"), lax.axis_index("seq")
    x, slot, core = lax.div(dp, 4), lax.rem(dp, 4), lax.rem(dp, 2)
    y_lo = lax.div(slot, 2)
    other = lax.rem(slot + 2, 4)
    after, before = (dp, lax.rem(seq + 1, 16)), (dp, lax.rem(seq + 15, 16))
    has_after, has_before = seq < 15, seq > 0
    spreads = lax.div(seq, 8) != lax.div(lax.rem(seq, 8), 4)
    beside = dp + 2 - 4 * y_lo
    above = (beside, lax.rem(seq + 8 * y_lo, 16))
    below = (beside, lax.rem(seq + 8 - 8 * y_lo, 16))
    partner = (dp + 1 - 2 * core, seq)
    across = [None] + [(lax.rem(dp + 4 * o, 16), seq) for o in range(1, 4)]

    def cols(c):
        return pl.ds(pl.multiple_of(c * CHUNK, CHUNK), CHUNK)

    def place(number):
        return pl.ds(pl.multiple_of(number * 128, 128), 128)

    def head(u):
        return pl.ds(pl.multiple_of(u * HEAD_DIM, HEAD_DIM), HEAD_DIM)

    def kv_load(c):
        return pltpu.make_async_copy(kv_in.at[:, :, cols(c)], kv_ref.at[:, :, cols(c)], kv_sem.at[c])

    load_tags = pltpu.make_async_copy(tags_in, tags_ref, in_sem.at[0])
    load_gy = pltpu.make_async_copy(gy_in, gy_ref, in_sem.at[1])
    load_w = pltpu.make_async_copy(w_in, wg.at[:, :, place(slot)], in_sem.at[2])
    load_seg = pltpu.make_async_copy(seg_in, seg_ref, in_sem.at[3])
    load_q = pltpu.make_async_copy(q_in, q_ref, in_sem.at[4])
    load_tags.start()
    load_gy.start()
    for c in range(2):
        kv_load(c).start()
    load_w.start()
    load_seg.start()
    load_q.start()
    for c in range(2, COUNT):
        kv_load(c).start()
    barrier = pltpu.get_barrier_semaphore()
    for peer in (after, before, above, below, partner, *across[1:]):
        pl.semaphore_signal(barrier, inc=1, device_id=peer, device_id_type=MESH)
    pl.semaphore_wait(barrier, 8)

    def remote(src, dst, send, recv, to):
        return pltpu.make_async_remote_copy(
            src_ref=src, dst_ref=dst, send_sem=send, recv_sem=recv,
            device_id=to, device_id_type=MESH,
        )

    def tags_to(o):
        return remote(tags_ref, tagb.at[3 - o], s_tag.at[o - 1], r_tag.at[3 - o], across[o])

    def grad_to(o):
        part = pl.ds(pl.multiple_of(lax.rem(x + o, 4) * PART, PART), PART)
        return remote(gy_ref.at[:, part], gyb.at[3 - o], s_gy.at[o - 1], r_gy.at[3 - o], across[o])

    def weight_to(kind, c):
        piece = wg.at[:, cols(c), place(other if kind == 3 else slot)]
        to = (above, below, partner, partner)[kind]
        return remote(piece, piece, s_w.at[kind], r_w.at[max(kind - 1, 0), c], to)

    def partial_to(o, c):
        return remote(
            psend.at[o - 1, :, cols(c)], precv.at[3 - o, :, cols(c)],
            s_p.at[o - 1], r_p.at[3 - o, c], across[o],
        )

    def kv_to(kind, u):
        src, dst, to = (
            (kv_ref, near, after), (near, far, after), (sa, ra, before), (sb, rb, before)
        )[kind]
        return remote(
            src.at[:, :, head(u)], dst.at[:, :, head(u)], s_kv.at[kind], r_kv.at[kind, u], to
        )

    def send(kind, c):
        pl.when(has_after if kind < 2 else has_before)(lambda: kv_to(kind, c).start())

    def receive(kind, c):
        pl.when(has_before if kind < 2 else has_after)(lambda: kv_to(kind, c).wait_recv())

    load_tags.wait()
    load_gy.wait()
    for o in (2, 1, 3):
        tags_to(o).start()
        grad_to(o).start()
    for c in range(LEAD // 2):
        kv_load(c).wait()
        send(0, 2 * c)
        send(0, 2 * c + 1)
    load_w.wait()

    @pl.loop(0, COUNT)
    def _(c):
        @pl.when(spreads)
        def _():
            weight_to(0, c).start()
            weight_to(1, c).start()

        weight_to(2, c).start()

    @pl.when(jnp.logical_not(has_before))
    def _():
        near[...] = jnp.zeros_like(near)
        far[...] = jnp.zeros_like(far)

    @pl.when(jnp.logical_not(has_after))
    def _():
        ra[...] = jnp.zeros_like(ra)
        rb[...] = jnp.zeros_like(rb)

    load_seg.wait()
    own_row = seg_ref[:, place(seq)]
    for back in range(REACH, -1, -1):
        key_row = seg_ref[:, place(jnp.maximum(seq - back, 0))]
        same = down(key_row) == jnp.broadcast_to(own_row.astype(F32), (ROWS, ROWS))
        if back == 0:
            key = lax.broadcasted_iota(jnp.int32, (ROWS, ROWS), 0)
            query = lax.broadcasted_iota(jnp.int32, (ROWS, ROWS), 1)
            block = jnp.where(jnp.logical_and(same, key <= query), 0.0, NEG)
        else:
            block = jnp.where(same, jnp.where(seq >= back, 0.0, NEG).astype(F32), NEG)
        bias[(REACH - back) * ROWS : (REACH - back + 1) * ROWS, :] = block

    for r in range(4):
        if r > 0:
            tags_to(4 - r).wait_recv()
            grad_to(4 - r).wait_recv()
            text = down(tagb[r - 1]) == 1.0
        else:
            text = down(tags_ref[...]) == 1.0
        for j in range(4):
            if r > 0:
                block = gyb[r - 1, :, j * 128 : (j + 1) * 128]
            else:
                block = gy_ref[:, place(x * 4 + j)]
            block = block.astype(F32)
            rows = slice(r * ROWS, (r + 1) * ROWS)
            gm[rows, j * 128 : (j + 1) * 128] = jnp.where(text, block, 0.0).astype(BF16)
            gm[rows, PART + j * 128 : PART + (j + 1) * 128] = jnp.where(text, 0.0, block).astype(BF16)

    def relay(c):
        weight_to(0, c).wait_recv()
        weight_to(3, c).start()

    def project(c):
        weight_to(2, c).wait_recv()
        weight_to(3, c).wait_recv()
        total = lax.dot_general(
            gm[:, :PART], wg[1, cols(c), :], LAST, preferred_element_type=F32
        ) + lax.dot_general(gm[:, PART:], wg[0, cols(c), :], LAST, preferred_element_type=F32)
        pown[:, cols(c)] = total[:ROWS]
        for o in (2, 1, 3):
            psend[o - 1, :, cols(c)] = total[o * ROWS : (o + 1) * ROWS].astype(BF16)
            partial_to(o, c).start()

    def attend(u, first):
        if first:
            for o in range(1, 4):
                partial_to(o, lax.div(u, 2)).wait_recv()
        here = head(u)
        grad = pown[:, here]
        for r in range(3):
            grad = grad + precv[r, :, here].astype(F32)
        grad = grad.astype(BF16)
        query = q_ref[:, here]
        receive(1, u)
        keys = jnp.concatenate([far[0, :, here], near[0, :, here], kv_ref[0, :, here]], axis=0)
        values = jnp.concatenate([far[1, :, here], near[1, :, here], kv_ref[1, :, here]], axis=0)
        scores = lax.dot_general(keys, query, LAST, preferred_element_type=F32)
        scores = scores * SCALE + bias[...]
        raised = jnp.exp(scores - jnp.max(scores, axis=0, keepdims=True))
        dprob = lax.dot_general(values, grad, LAST, preferred_element_type=F32)
        share = 1.0 / jnp.sum(raised, axis=0, keepdims=True)
        probs = raised * share
        delta = jnp.sum(probs * dprob, axis=0, keepdims=True)
        dscore = (probs * (dprob - delta) * SCALE).astype(BF16)
        grad_k = jnp.dot(dscore, query, preferred_element_type=F32)
        grad_v = jnp.dot(probs.astype(BF16), grad, preferred_element_type=F32)
        sa[0, :, here] = grad_k[:ROWS].astype(BF16)
        sa[1, :, here] = grad_v[:ROWS].astype(BF16)
        send(2, u)
        for index, term in ((0, grad_k), (1, grad_v)):
            t1[index, :, here] = term[ROWS : 2 * ROWS]
            t0[index, :, here] = term[2 * ROWS :]
        grad_q = lax.dot_general(dscore, keys, FIRST, preferred_element_type=F32)
        gq_ref[:, here] = grad_q.astype(BF16)

    def fold(u):
        receive(2, u)
        sb[:, :, head(u)] = (ra[:, :, head(u)].astype(F32) + t1[:, :, head(u)]).astype(BF16)
        send(3, u)

    def finish(u):
        receive(3, u)
        gkv_ref[:, :, head(u)] = (rb[:, :, head(u)].astype(F32) + t0[:, :, head(u)]).astype(BF16)

    def extend(u):
        receive(0, u)
        send(1, u)

    load_q.wait()
    for c in range(LEAD // 2, COUNT):
        kv_load(c).wait()
    relay(0)
    extend(0)
    send(0, LEAD)
    relay(1)
    project(0)

    @pl.loop(0, (HEADS + BACK + HOME + 1) // 2)
    def _(j):
        for b in range(2):
            u = 2 * j + b
            pl.when(jnp.logical_and(u >= 1, u < HEADS))(lambda: extend(u))
            pl.when(jnp.logical_and(u >= 1, u + LEAD < HEADS))(lambda: send(0, u + LEAD))
            if b == 0:
                pl.when(j + 2 < COUNT)(lambda: relay(j + 2))
                pl.when(j + 1 < COUNT)(lambda: project(j + 1))
            pl.when(jnp.logical_and(u >= 1, u <= HEADS))(lambda: attend(u - 1, b == 1))
            pl.when(jnp.logical_and(u >= BACK, u < HEADS + BACK))(lambda: fold(u - BACK))
            last = BACK + HOME
            pl.when(jnp.logical_and(u >= last, u < HEADS + last))(lambda: finish(u - last))

    for o in range(1, 4):
        tags_to(o).wait_send()
        grad_to(o).wait_send()

    whole = wg.at[:, :, place(slot)]
    for kind in range(4):
        done = remote(whole, whole, s_w.at[kind], r_w.at[0, 0], partner)
        if kind < 2:
            pl.when(spreads)(done.wait_send)
        else:
            done.wait_send()
        done = remote(near, far, s_kv.at[kind], r_kv.at[0, 0], after)
        pl.when(has_after if kind < 2 else has_before)(done.wait_send)
    for o in range(1, 4):
        remote(psend.at[o - 1], precv.at[3 - o], s_p.at[o - 1], r_p.at[0, 0], across[o]).wait_send()


def shards(query, key_value, grad_y, tags, segments, out_weight):
    vmem = pl.BlockSpec(memory_space=pltpu.VMEM)
    dma = pltpu.SemaphoreType.DMA
    held = [
        pltpu.with_memory_space_constraint(array, pltpu.HBM)
        for array in (query[0], key_value[:, 0], grad_y[0], tags, segments, out_weight)
    ]
    pair = (2, ROWS, WIDTH)
    grad_q, grad_kv = pl.pallas_call(
        kernel,
        out_shape=(
            jax.ShapeDtypeStruct((ROWS, WIDTH), BF16),
            jax.ShapeDtypeStruct(pair, BF16),
        ),
        in_specs=[pl.BlockSpec(memory_space=pltpu.HBM)] * 6,
        out_specs=(vmem, vmem),
        scratch_shapes=[
            pltpu.VMEM((ROWS, WIDTH), BF16),
            pltpu.VMEM(pair, BF16),
            pltpu.VMEM((ROWS, WIDTH), BF16),
            pltpu.VMEM((1, ROWS), jnp.int32),
            pltpu.VMEM((1, WIDTH), jnp.int32),
            pltpu.VMEM((2, WIDTH, PART), BF16),
            pltpu.VMEM((3, ROWS, PART), BF16),
            pltpu.VMEM((3, 1, ROWS), jnp.int32),
            pltpu.VMEM((4 * ROWS, 2 * PART), BF16),
            pltpu.VMEM((3, ROWS, WIDTH), BF16),
            pltpu.VMEM((3, ROWS, WIDTH), BF16),
            pltpu.VMEM((ROWS, WIDTH), F32),
            pltpu.VMEM(pair, BF16),
            pltpu.VMEM(pair, BF16),
            pltpu.VMEM(((REACH + 1) * ROWS, ROWS), F32),
            pltpu.VMEM(pair, F32),
            pltpu.VMEM(pair, F32),
            pltpu.VMEM(pair, BF16),
            pltpu.VMEM(pair, BF16),
            pltpu.VMEM(pair, BF16),
            pltpu.VMEM(pair, BF16),
            dma((5,)), dma((COUNT,)),
            dma((3,)), dma((3,)), dma((3,)), dma((3,)),
            dma((4,)), dma((3, COUNT)),
            dma((3,)), dma((3, COUNT)),
            dma((4,)), dma((4, HEADS)),
        ],
        compiler_params=pltpu.CompilerParams(
            collective_id=1, has_side_effects=True, vmem_limit_bytes=48 << 20
        ),
        name="mixed_backward",
    )(*held)
    return grad_q[None], grad_kv[:, None]


def solution(mesh):
    return jax.shard_map(
        shards,
        mesh=mesh,
        in_specs=(
            P("dp", "seq", None),
            P(None, "dp", "seq", None),
            P("dp", "seq", None),
            P("dp", "seq"),
            P("dp", None),
            P(None, None, "dp"),
        ),
        out_specs=(P("dp", "seq", None), P(None, "dp", "seq", None)),
        check_vma=False,
    )
```

```python
import jax
import jax.numpy as jnp
from jax import lax
from jax.experimental import pallas as pl
from jax.experimental.pallas import tpu as pltpu
from jax.sharding import PartitionSpec as P

HEAD_DIM = 128
ROWS = 128
WIDTH = 2048
PART = 512
CHUNK = 256
COUNT = WIDTH // CHUNK
HEADS = WIDTH // HEAD_DIM
LEAD = 16
NEXT = 3
BACK = 7
HOME = 12
SCALE = HEAD_DIM ** -0.5
NEG = -1e30
F32 = jnp.float32
BF16 = jnp.bfloat16
MESH = pl.DeviceIdType.MESH
LAST = (((1,), (1,)), ((), ()))
FIRST = (((0,), (0,)), ((), ()))


def down(row):
    return jnp.broadcast_to(row.astype(F32), (ROWS, ROWS)).T


def kernel(
    q_in, kv_in, gy_in, tags_in, seg_in, w_in, gq_ref, gkv_ref,
    q_ref, kv_ref, gy_ref, tags_ref, seg_ref, wg, gyb, tagb, gm, psend, precv, pown, bias,
    near, q_next, grad_own, grad_next, raised, dprob, up_own, down_own, up_got, down_got,
    q_part, q_got, q_sum, kv_part, kv_got, kv_sum,
    in_sem, kv_sem, s_gy, r_gy, s_tag, r_tag, s_w, r_w, s_p, r_p, s_kv, r_kv,
):
    dp, seq = lax.axis_index("dp"), lax.axis_index("seq")
    x, slot, core = lax.div(dp, 4), lax.rem(dp, 4), lax.rem(dp, 2)
    y_lo = lax.div(slot, 2)
    other = lax.rem(slot + 2, 4)
    after, before = (dp, lax.rem(seq + 1, 16)), (dp, lax.rem(seq + 15, 16))
    has_after, has_before = seq < 15, seq > 0
    spreads = lax.div(seq, 8) != lax.div(lax.rem(seq, 8), 4)
    beside = dp + 2 - 4 * y_lo
    above = (beside, lax.rem(seq + 8 * y_lo, 16))
    below = (beside, lax.rem(seq + 8 - 8 * y_lo, 16))
    partner = (dp + 1 - 2 * core, seq)
    across = [None] + [(lax.rem(dp + 4 * o, 16), seq) for o in range(1, 4)]

    def cols(c):
        return pl.ds(pl.multiple_of(c * CHUNK, CHUNK), CHUNK)

    def place(number):
        return pl.ds(pl.multiple_of(number * 128, 128), 128)

    def head(u):
        return pl.ds(pl.multiple_of(u * HEAD_DIM, HEAD_DIM), HEAD_DIM)

    def kv_load(c):
        return pltpu.make_async_copy(kv_in.at[:, :, cols(c)], kv_ref.at[:, :, cols(c)], kv_sem.at[c])

    load_tags = pltpu.make_async_copy(tags_in, tags_ref, in_sem.at[0])
    load_gy = pltpu.make_async_copy(gy_in, gy_ref, in_sem.at[1])
    load_w = pltpu.make_async_copy(w_in, wg.at[:, :, place(slot)], in_sem.at[2])
    load_seg = pltpu.make_async_copy(seg_in, seg_ref, in_sem.at[3])
    load_q = pltpu.make_async_copy(q_in, q_ref, in_sem.at[4])
    load_tags.start()
    load_gy.start()
    for c in range(2):
        kv_load(c).start()
    load_w.start()
    load_seg.start()
    load_q.start()
    for c in range(2, COUNT):
        kv_load(c).start()
    barrier = pltpu.get_barrier_semaphore()
    for peer in (after, before, above, below, partner, *across[1:]):
        pl.semaphore_signal(barrier, inc=1, device_id=peer, device_id_type=MESH)
    pl.semaphore_wait(barrier, 8)

    def remote(src, dst, send, recv, to):
        return pltpu.make_async_remote_copy(
            src_ref=src, dst_ref=dst, send_sem=send, recv_sem=recv,
            device_id=to, device_id_type=MESH,
        )

    def tags_to(o):
        return remote(tags_ref, tagb.at[3 - o], s_tag.at[o - 1], r_tag.at[3 - o], across[o])

    def grad_to(o):
        part = pl.ds(pl.multiple_of(lax.rem(x + o, 4) * PART, PART), PART)
        return remote(gy_ref.at[:, part], gyb.at[3 - o], s_gy.at[o - 1], r_gy.at[3 - o], across[o])

    def weight_to(kind, c):
        piece = wg.at[:, cols(c), place(other if kind == 3 else slot)]
        to = (above, below, partner, partner)[kind]
        return remote(piece, piece, s_w.at[kind], r_w.at[max(kind - 1, 0), c], to)

    def partial_to(o, c):
        return remote(
            psend.at[o - 1, :, cols(c)], precv.at[3 - o, :, cols(c)],
            s_p.at[o - 1], r_p.at[3 - o, c], across[o],
        )

    moves = (
        (kv_ref, near, after),
        (q_ref, q_next, before),
        (grad_own, grad_next, before),
        (up_own, up_got, before),
        (down_own, down_got, after),
        (q_part, q_got, after),
        (kv_part, kv_got, before),
    )
    forward = (True, False, False, False, True, True, False)

    def move(kind, u):
        src, dst, to = moves[kind]
        if kind in (3, 4):
            src, dst = src.at[u], dst.at[u]
        elif kind in (0, 6):
            src, dst = src.at[:, :, head(u)], dst.at[:, :, head(u)]
        else:
            src, dst = src.at[:, head(u)], dst.at[:, head(u)]
        return remote(src, dst, s_kv.at[kind], r_kv.at[kind, u], to)

    def send(kind, c):
        pl.when(has_after if forward[kind] else has_before)(lambda: move(kind, c).start())

    def receive(kind, c):
        pl.when(has_before if forward[kind] else has_after)(lambda: move(kind, c).wait_recv())

    load_tags.wait()
    load_gy.wait()
    for o in (2, 1, 3):
        tags_to(o).start()
        grad_to(o).start()
    for c in range(LEAD // 2):
        kv_load(c).wait()
        send(0, 2 * c)
        send(0, 2 * c + 1)
    load_q.wait()

    @pl.loop(0, HEADS)
    def _(u):
        send(1, u)

    load_w.wait()

    @pl.loop(0, COUNT)
    def _(c):
        @pl.when(spreads)
        def _():
            weight_to(0, c).start()
            weight_to(1, c).start()

        weight_to(2, c).start()

    first_rows = lax.broadcasted_iota(jnp.int32, (HEADS, 8, ROWS), 1)

    @pl.when(jnp.logical_not(has_before))
    def _():
        near[...] = jnp.zeros_like(near)
        q_got[...] = jnp.zeros_like(q_got)
        down_got[...] = jnp.where(first_rows == 0, NEG, 0.0).astype(F32)

    @pl.when(jnp.logical_not(has_after))
    def _():
        q_next[...] = jnp.zeros_like(q_next)
        grad_next[...] = jnp.zeros_like(grad_next)
        kv_got[...] = jnp.zeros_like(kv_got)
        up_got[...] = jnp.ones_like(up_got)

    load_seg.wait()
    behind, ahead = jnp.maximum(seq - 1, 0), jnp.minimum(seq + 1, 15)
    near_valid = jnp.where(has_before, 0.0, NEG).astype(F32)
    next_valid = jnp.where(has_after, near_valid, NEG).astype(F32)
    for part, (key_block, query_block) in enumerate(((behind, ahead), (behind, seq), (seq, seq))):
        query_row = seg_ref[:, place(query_block)].astype(F32)
        same = down(seg_ref[:, place(key_block)]) == jnp.broadcast_to(query_row, (ROWS, ROWS))
        if part == 2:
            key = lax.broadcasted_iota(jnp.int32, (ROWS, ROWS), 0)
            query = lax.broadcasted_iota(jnp.int32, (ROWS, ROWS), 1)
            block = jnp.where(jnp.logical_and(same, key <= query), 0.0, NEG)
        else:
            block = jnp.where(same, (next_valid, near_valid)[part], NEG)
        bias[part * ROWS : (part + 1) * ROWS, :] = block

    for r in range(4):
        if r > 0:
            tags_to(4 - r).wait_recv()
            grad_to(4 - r).wait_recv()
            text = down(tagb[r - 1]) == 1.0
        else:
            text = down(tags_ref[...]) == 1.0
        for j in range(4):
            if r > 0:
                block = gyb[r - 1, :, j * 128 : (j + 1) * 128]
            else:
                block = gy_ref[:, place(x * 4 + j)]
            block = block.astype(F32)
            rows = slice(r * ROWS, (r + 1) * ROWS)
            gm[rows, j * 128 : (j + 1) * 128] = jnp.where(text, block, 0.0).astype(BF16)
            gm[rows, PART + j * 128 : PART + (j + 1) * 128] = jnp.where(text, 0.0, block).astype(BF16)

    def relay(c):
        weight_to(0, c).wait_recv()
        weight_to(3, c).start()

    def project(c):
        weight_to(2, c).wait_recv()
        weight_to(3, c).wait_recv()
        total = lax.dot_general(
            gm[:, :PART], wg[1, cols(c), :], LAST, preferred_element_type=F32
        ) + lax.dot_general(gm[:, PART:], wg[0, cols(c), :], LAST, preferred_element_type=F32)
        pown[:, cols(c)] = total[:ROWS]
        for o in (2, 1, 3):
            psend[o - 1, :, cols(c)] = total[o * ROWS : (o + 1) * ROWS].astype(BF16)
            partial_to(o, c).start()

    def collect(u, first):
        if first:
            for o in range(1, 4):
                partial_to(o, lax.div(u, 2)).wait_recv()
        grad = pown[:, head(u)]
        for r in range(3):
            grad = grad + precv[r, :, head(u)].astype(F32)
        grad_own[:, head(u)] = grad.astype(BF16)
        send(2, u)

    row = lax.broadcasted_iota(jnp.int32, (8, ROWS), 0)

    def partial_rows(keys, values, query, grad, mask):
        scores = lax.dot_general(keys, query, LAST, preferred_element_type=F32) * SCALE + mask
        top = jnp.max(scores, axis=0, keepdims=True)
        power = jnp.exp(scores - top)
        grads = lax.dot_general(values, grad, LAST, preferred_element_type=F32)
        total = jnp.sum(power, axis=0, keepdims=True)
        dot = jnp.sum(power * grads, axis=0, keepdims=True)
        return power, grads, jnp.where(row == 0, top, jnp.where(row == 1, total, dot))

    def score(u):
        here = head(u)
        for kind in (0, 1, 2):
            receive(kind, u)
        power, grads, down_own[u] = partial_rows(
            near[0, :, here], near[1, :, here], q_next[:, here], grad_next[:, here], bias[:ROWS]
        )
        send(4, u)
        raised[u, :ROWS], dprob[u, :ROWS] = power, grads
        power, grads, up_own[u] = partial_rows(
            jnp.concatenate([near[0, :, here], kv_ref[0, :, here]], axis=0),
            jnp.concatenate([near[1, :, here], kv_ref[1, :, here]], axis=0),
            q_ref[:, here], grad_own[:, here], bias[ROWS:],
        )
        send(3, u)
        raised[u, ROWS:], dprob[u, ROWS:] = power, grads

    def merge(mine, got, u):
        top, total, dot = (mine[u, r : r + 1, :] for r in range(3))
        top_got, total_got, dot_got = (got[u, r : r + 1, :] for r in range(3))
        both = jnp.maximum(top, top_got)
        weight, weight_got = jnp.exp(top - both), jnp.exp(top_got - both)
        share = 1.0 / (total * weight + total_got * weight_got)
        return weight * share, (dot * weight + dot_got * weight_got) * share

    def grads(u):
        here = head(u)
        receive(3, u)
        receive(4, u)
        factor, delta = merge(down_own, up_got, u)
        probs = raised[u, :ROWS] * factor
        dscore_next = (probs * (dprob[u, :ROWS] - delta) * SCALE).astype(BF16)
        probs_next = probs.astype(BF16)
        key_near = near[0, :, here]
        q_part[:, here] = lax.dot_general(
            dscore_next, key_near, FIRST, preferred_element_type=F32
        ).astype(BF16)
        send(5, u)
        factor, delta = merge(up_own, down_got, u)
        probs = raised[u, ROWS:] * factor
        dscore = (probs * (dprob[u, ROWS:] - delta) * SCALE).astype(BF16)
        probs = probs.astype(BF16)
        query, grad = q_ref[:, here], grad_own[:, here]
        kv_part[0, :, here] = jnp.dot(
            jnp.concatenate([dscore[:ROWS], dscore_next], axis=1),
            jnp.concatenate([query, q_next[:, here]], axis=0),
            preferred_element_type=F32,
        ).astype(BF16)
        kv_part[1, :, here] = jnp.dot(
            jnp.concatenate([probs[:ROWS], probs_next], axis=1),
            jnp.concatenate([grad, grad_next[:, here]], axis=0),
            preferred_element_type=F32,
        ).astype(BF16)
        send(6, u)
        kv_sum[0, :, here] = jnp.dot(dscore[ROWS:], query, preferred_element_type=F32)
        kv_sum[1, :, here] = jnp.dot(probs[ROWS:], grad, preferred_element_type=F32)
        q_sum[:, here] = lax.dot_general(
            dscore, jnp.concatenate([key_near, kv_ref[0, :, here]], axis=0), FIRST,
            preferred_element_type=F32,
        )

    def finish(u):
        here = head(u)
        receive(5, u)
        gq_ref[:, here] = (q_got[:, here].astype(F32) + q_sum[:, here]).astype(BF16)
        receive(6, u)
        gkv_ref[:, :, here] = (kv_got[:, :, here].astype(F32) + kv_sum[:, :, here]).astype(BF16)

    for c in range(LEAD // 2, COUNT):
        kv_load(c).wait()
    relay(0)
    project(0)
    relay(1)
    project(1)
    relay(2)

    @pl.loop(0, (HEADS + HOME + 1) // 2)
    def _(j):
        for b in range(2):
            u = 2 * j + b
            pl.when(u + LEAD < HEADS)(lambda: send(0, u + LEAD))
            pl.when(u < HEADS)(lambda: collect(u, b == 0))
            if b == 0:
                pl.when(j + 3 < COUNT)(lambda: relay(j + 3))
                pl.when(j + 2 < COUNT)(lambda: project(j + 2))
            pl.when(jnp.logical_and(u >= NEXT, u < HEADS + NEXT))(lambda: score(u - NEXT))
            pl.when(jnp.logical_and(u >= BACK, u < HEADS + BACK))(lambda: grads(u - BACK))
            pl.when(jnp.logical_and(u >= HOME, u < HEADS + HOME))(lambda: finish(u - HOME))

    for o in range(1, 4):
        tags_to(o).wait_send()
        grad_to(o).wait_send()

    whole = wg.at[:, :, place(slot)]
    for kind in range(4):
        done = remote(whole, whole, s_w.at[kind], r_w.at[0, 0], partner)
        if kind < 2:
            pl.when(spreads)(done.wait_send)
        else:
            done.wait_send()
    for kind, (src, dst, to) in enumerate(moves):
        done = remote(src, dst, s_kv.at[kind], r_kv.at[0, 0], to)
        pl.when(has_after if forward[kind] else has_before)(done.wait_send)
    for o in range(1, 4):
        remote(psend.at[o - 1], precv.at[3 - o], s_p.at[o - 1], r_p.at[0, 0], across[o]).wait_send()


def shards(query, key_value, grad_y, tags, segments, out_weight):
    vmem = pl.BlockSpec(memory_space=pltpu.VMEM)
    dma = pltpu.SemaphoreType.DMA
    held = [
        pltpu.with_memory_space_constraint(array, pltpu.HBM)
        for array in (query[0], key_value[:, 0], grad_y[0], tags, segments, out_weight)
    ]
    pair = (2, ROWS, WIDTH)
    grad_q, grad_kv = pl.pallas_call(
        kernel,
        out_shape=(
            jax.ShapeDtypeStruct((ROWS, WIDTH), BF16),
            jax.ShapeDtypeStruct(pair, BF16),
        ),
        in_specs=[pl.BlockSpec(memory_space=pltpu.HBM)] * 6,
        out_specs=(vmem, vmem),
        scratch_shapes=[
            pltpu.VMEM((ROWS, WIDTH), BF16),
            pltpu.VMEM(pair, BF16),
            pltpu.VMEM((ROWS, WIDTH), BF16),
            pltpu.VMEM((1, ROWS), jnp.int32),
            pltpu.VMEM((1, WIDTH), jnp.int32),
            pltpu.VMEM((2, WIDTH, PART), BF16),
            pltpu.VMEM((3, ROWS, PART), BF16),
            pltpu.VMEM((3, 1, ROWS), jnp.int32),
            pltpu.VMEM((4 * ROWS, 2 * PART), BF16),
            pltpu.VMEM((3, ROWS, WIDTH), BF16),
            pltpu.VMEM((3, ROWS, WIDTH), BF16),
            pltpu.VMEM((ROWS, WIDTH), F32),
            pltpu.VMEM((3 * ROWS, ROWS), F32),
            pltpu.VMEM(pair, BF16),
            pltpu.VMEM((ROWS, WIDTH), BF16),
            pltpu.VMEM((ROWS, WIDTH), BF16),
            pltpu.VMEM((ROWS, WIDTH), BF16),
            pltpu.VMEM((HEADS, 3 * ROWS, ROWS), F32),
            pltpu.VMEM((HEADS, 3 * ROWS, ROWS), F32),
            *[pltpu.VMEM((HEADS, 8, ROWS), F32)] * 4,
            pltpu.VMEM((ROWS, WIDTH), BF16),
            pltpu.VMEM((ROWS, WIDTH), BF16),
            pltpu.VMEM((ROWS, WIDTH), F32),
            pltpu.VMEM(pair, BF16),
            pltpu.VMEM(pair, BF16),
            pltpu.VMEM(pair, F32),
            dma((5,)), dma((COUNT,)),
            dma((3,)), dma((3,)), dma((3,)), dma((3,)),
            dma((4,)), dma((3, COUNT)),
            dma((3,)), dma((3, COUNT)),
            dma((7,)), dma((7, HEADS)),
        ],
        compiler_params=pltpu.CompilerParams(
            collective_id=1, has_side_effects=True, vmem_limit_bytes=48 << 20
        ),
        name="mixed_backward",
    )(*held)
    return grad_q[None], grad_kv[:, None]


def solution(mesh):
    return jax.shard_map(
        shards,
        mesh=mesh,
        in_specs=(
            P("dp", "seq", None),
            P(None, "dp", "seq", None),
            P("dp", "seq", None),
            P("dp", "seq"),
            P("dp", None),
            P(None, None, "dp"),
        ),
        out_specs=(P("dp", "seq", None), P(None, "dp", "seq", None)),
        check_vma=False,
    )
```

```python
import jax
import jax.numpy as jnp
from jax import lax
from jax.experimental import pallas as pl
from jax.experimental.pallas import tpu as pltpu
from jax.sharding import PartitionSpec as P

HEAD_DIM = 128
ROWS = 128
WIDTH = 2048
PART = 512
CHUNK = 256
COUNT = WIDTH // CHUNK
HEADS = WIDTH // HEAD_DIM
LEAD = 8
EARLY = 6
NEXT = 3
BACK = 7
HOME = 11
SCALE = HEAD_DIM ** -0.5
NEG = -1e30
F32 = jnp.float32
BF16 = jnp.bfloat16
MESH = pl.DeviceIdType.MESH
LAST = (((1,), (1,)), ((), ()))
FIRST = (((0,), (0,)), ((), ()))


def down(row):
    return jnp.broadcast_to(row.astype(F32), (ROWS, ROWS)).T


def kernel(
    q_in, kv_in, gy_in, tags_in, seg_in, w_in, gq_ref, gkv_ref,
    q_ref, kv_ref, gy_ref, tags_ref, seg_ref, wg, gyb, tagb, gm, psend, precv, pown, bias,
    near, q_next, grad_own, grad_next, raised, dprob, up_own, down_own, up_got, down_got,
    up_delta, down_delta, up_delta_got, down_delta_got, q_part, q_got, q_sum, kv_part, kv_got, kv_sum,
    in_sem, kv_sem, s_gy, r_gy, s_tag, r_tag, s_w, r_w, s_p, r_p, s_kv, r_kv,
):
    dp, seq = lax.axis_index("dp"), lax.axis_index("seq")
    x, slot, core = lax.div(dp, 4), lax.rem(dp, 4), lax.rem(dp, 2)
    y_lo = lax.div(slot, 2)
    other = lax.rem(slot + 2, 4)
    after, before = (dp, lax.rem(seq + 1, 16)), (dp, lax.rem(seq + 15, 16))
    has_after, has_before = seq < 15, seq > 0
    spreads = lax.div(seq, 8) != lax.div(lax.rem(seq, 8), 4)
    beside = dp + 2 - 4 * y_lo
    above = (beside, lax.rem(seq + 8 * y_lo, 16))
    below = (beside, lax.rem(seq + 8 - 8 * y_lo, 16))
    partner = (dp + 1 - 2 * core, seq)
    across = [None] + [(lax.rem(dp + 4 * o, 16), seq) for o in range(1, 4)]

    def cols(c):
        return pl.ds(pl.multiple_of(c * CHUNK, CHUNK), CHUNK)

    def place(number):
        return pl.ds(pl.multiple_of(number * 128, 128), 128)

    def head(u):
        return pl.ds(pl.multiple_of(u * HEAD_DIM, HEAD_DIM), HEAD_DIM)

    def kv_load(c):
        return pltpu.make_async_copy(kv_in.at[:, :, cols(c)], kv_ref.at[:, :, cols(c)], kv_sem.at[c])

    load_tags = pltpu.make_async_copy(tags_in, tags_ref, in_sem.at[0])
    load_gy = pltpu.make_async_copy(gy_in, gy_ref, in_sem.at[1])
    load_w = pltpu.make_async_copy(w_in, wg.at[:, :, place(slot)], in_sem.at[2])
    load_seg = pltpu.make_async_copy(seg_in, seg_ref, in_sem.at[3])
    load_q = pltpu.make_async_copy(q_in, q_ref, in_sem.at[4])
    load_tags.start()
    load_gy.start()
    for c in range(2):
        kv_load(c).start()
    load_w.start()
    load_seg.start()
    load_q.start()
    for c in range(2, COUNT):
        kv_load(c).start()
    barrier = pltpu.get_barrier_semaphore()
    for peer in (after, before, above, below, partner, *across[1:]):
        pl.semaphore_signal(barrier, inc=1, device_id=peer, device_id_type=MESH)
    pl.semaphore_wait(barrier, 8)

    def remote(src, dst, send, recv, to):
        return pltpu.make_async_remote_copy(
            src_ref=src, dst_ref=dst, send_sem=send, recv_sem=recv,
            device_id=to, device_id_type=MESH,
        )

    def tags_to(o):
        return remote(tags_ref, tagb.at[3 - o], s_tag.at[o - 1], r_tag.at[3 - o], across[o])

    def grad_to(o):
        part = pl.ds(pl.multiple_of(lax.rem(x + o, 4) * PART, PART), PART)
        return remote(gy_ref.at[:, part], gyb.at[3 - o], s_gy.at[o - 1], r_gy.at[3 - o], across[o])

    def weight_to(kind, c):
        piece = wg.at[:, cols(c), place(other if kind == 3 else slot)]
        to = (above, below, partner, partner)[kind]
        return remote(piece, piece, s_w.at[kind], r_w.at[max(kind - 1, 0), c], to)

    def partial_to(o, u):
        return remote(
            psend.at[o - 1, :, head(u)], precv.at[3 - o, :, head(u)],
            s_p.at[o - 1], r_p.at[3 - o, u], across[o],
        )

    moves = (
        (kv_ref, near, after),
        (q_ref, q_next, before),
        (grad_own, grad_next, before),
        (up_own, up_got, before),
        (down_own, down_got, after),
        (q_part, q_got, after),
        (kv_part.at[1], kv_got.at[1], before),
        (kv_part.at[0], kv_got.at[0], before),
        (up_delta, up_delta_got, before),
        (down_delta, down_delta_got, after),
    )
    forward = (True, False, False, False, True, True, False, False, False, True)

    def move(kind, u):
        src, dst, to = moves[kind]
        if kind in (3, 4, 8, 9):
            src, dst = src.at[u], dst.at[u]
        elif kind == 0:
            src, dst = src.at[:, :, head(u)], dst.at[:, :, head(u)]
        else:
            src, dst = src.at[:, head(u)], dst.at[:, head(u)]
        return remote(src, dst, s_kv.at[kind], r_kv.at[kind, u], to)

    def send(kind, c):
        pl.when(has_after if forward[kind] else has_before)(lambda: move(kind, c).start())

    def receive(kind, c):
        pl.when(has_before if forward[kind] else has_after)(lambda: move(kind, c).wait_recv())

    load_tags.wait()
    load_gy.wait()
    for o in (2, 1, 3):
        tags_to(o).start()
        grad_to(o).start()
    for c in range(LEAD // 2):
        kv_load(c).wait()
        send(0, 2 * c)
        send(0, 2 * c + 1)
    load_q.wait()

    @pl.loop(0, HEADS)
    def _(u):
        send(1, u)

    load_w.wait()

    @pl.loop(0, COUNT)
    def _(c):
        @pl.when(spreads)
        def _():
            weight_to(0, c).start()
            weight_to(1, c).start()

        weight_to(2, c).start()

    first_rows = lax.broadcasted_iota(jnp.int32, (HEADS, 2, ROWS), 1)

    @pl.when(jnp.logical_not(has_before))
    def _():
        near[...] = jnp.zeros_like(near)
        q_got[...] = jnp.zeros_like(q_got)
        down_got[...] = jnp.where(first_rows == 0, NEG, 0.0).astype(F32)
        down_delta_got[...] = jnp.zeros_like(down_delta_got)

    @pl.when(jnp.logical_not(has_after))
    def _():
        q_next[...] = jnp.zeros_like(q_next)
        grad_next[...] = jnp.zeros_like(grad_next)
        kv_got[...] = jnp.zeros_like(kv_got)
        up_got[...] = jnp.ones_like(up_got)
        up_delta_got[...] = jnp.zeros_like(up_delta_got)

    load_seg.wait()
    behind, ahead = jnp.maximum(seq - 1, 0), jnp.minimum(seq + 1, 15)
    near_valid = jnp.where(has_before, 0.0, NEG).astype(F32)
    next_valid = jnp.where(has_after, near_valid, NEG).astype(F32)
    for part, (key_block, query_block) in enumerate(((behind, ahead), (behind, seq), (seq, seq))):
        query_row = seg_ref[:, place(query_block)].astype(F32)
        same = down(seg_ref[:, place(key_block)]) == jnp.broadcast_to(query_row, (ROWS, ROWS))
        if part == 2:
            key = lax.broadcasted_iota(jnp.int32, (ROWS, ROWS), 0)
            query = lax.broadcasted_iota(jnp.int32, (ROWS, ROWS), 1)
            block = jnp.where(jnp.logical_and(same, key <= query), 0.0, NEG)
        else:
            block = jnp.where(same, (next_valid, near_valid)[part], NEG)
        bias[part * ROWS : (part + 1) * ROWS, :] = block

    def relay(c):
        weight_to(0, c).wait_recv()
        weight_to(3, c).start()

    def project(c):
        weight_to(2, c).wait_recv()
        weight_to(3, c).wait_recv()
        total = lax.dot_general(
            gm[:, :PART], wg[1, cols(c), :], LAST, preferred_element_type=F32
        ) + lax.dot_general(gm[:, PART:], wg[0, cols(c), :], LAST, preferred_element_type=F32)
        pown[:, cols(c)] = total[:ROWS]
        for o in (2, 1, 3):
            psend[o - 1, :, cols(c)] = total[o * ROWS : (o + 1) * ROWS].astype(BF16)
        for h in range(2):
            for o in (2, 1, 3):
                partial_to(o, 2 * c + h).start()

    def collect(u):
        for o in range(1, 4):
            partial_to(o, u).wait_recv()
        grad = pown[:, head(u)]
        for r in range(3):
            grad = grad + precv[r, :, head(u)].astype(F32)
        grad_own[:, head(u)] = grad.astype(BF16)
        send(2, u)

    row = lax.broadcasted_iota(jnp.int32, (2, ROWS), 0)

    def partial_rows(keys, query, mask):
        scores = lax.dot_general(keys, query, LAST, preferred_element_type=F32) * SCALE + mask
        top = jnp.max(scores, axis=0, keepdims=True)
        power = jnp.exp(scores - top)
        return power, jnp.where(row == 0, top, jnp.sum(power, axis=0, keepdims=True))

    def score(u):
        here = head(u)
        receive(0, u)
        pl.when(u + LEAD < HEADS)(lambda: send(0, u + LEAD))
        receive(1, u)
        raised[u, :ROWS], down_own[u] = partial_rows(near[0, :, here], q_next[:, here], bias[:ROWS])
        send(4, u)
        keys = jnp.concatenate([near[0, :, here], kv_ref[0, :, here]], axis=0)
        raised[u, ROWS:], up_own[u] = partial_rows(keys, q_ref[:, here], bias[ROWS:])
        send(3, u)

    def merge(mine, got, u):
        top, total = (mine[u, r : r + 1, :] for r in range(2))
        top_got, total_got = (got[u, r : r + 1, :] for r in range(2))
        both = jnp.maximum(top, top_got)
        weight, weight_got = jnp.exp(top - both), jnp.exp(top_got - both)
        return weight / (total * weight + total_got * weight_got)

    def weigh(u):
        here = head(u)
        for kind in (2, 3, 4):
            receive(kind, u)
        grad, grad_ahead = grad_own[:, here], grad_next[:, here]
        value_near, value_own = near[1, :, here], kv_ref[1, :, here]
        ahead_grads = lax.dot_general(value_near, grad_ahead, LAST, preferred_element_type=F32)
        ahead_probs = raised[u, :ROWS] * merge(down_own, up_got, u)
        total = jnp.sum(ahead_probs * ahead_grads, axis=0, keepdims=True)
        down_delta[u] = total
        send(9, u)
        values = jnp.concatenate([value_near, value_own], axis=0)
        grads = lax.dot_general(values, grad, LAST, preferred_element_type=F32)
        probs = raised[u, ROWS:] * merge(up_own, down_got, u)
        up_delta[u] = jnp.sum(probs * grads, axis=0, keepdims=True)
        send(8, u)
        raised[u, :ROWS], raised[u, ROWS:] = ahead_probs, probs
        dprob[u, :ROWS], dprob[u, ROWS:] = ahead_grads, grads
        probs = probs.astype(BF16)
        kv_part[1, :, here] = jnp.dot(
            jnp.concatenate([probs[:ROWS], ahead_probs.astype(BF16)], axis=1),
            jnp.concatenate([grad, grad_ahead], axis=0),
            preferred_element_type=F32,
        ).astype(BF16)
        send(6, u)
        kv_sum[1, :, here] = jnp.dot(probs[ROWS:], grad, preferred_element_type=F32)

    def grads(u):
        here = head(u)
        receive(8, u)
        receive(9, u)
        delta = down_delta[u] + up_delta_got[u]
        ahead = (raised[u, :ROWS] * (dprob[u, :ROWS] - delta) * SCALE).astype(BF16)
        query, key_near = q_ref[:, here], near[0, :, here]
        q_part[:, here] = lax.dot_general(
            ahead, key_near, FIRST, preferred_element_type=F32
        ).astype(BF16)
        send(5, u)
        delta = up_delta[u] + down_delta_got[u]
        dscore = (raised[u, ROWS:] * (dprob[u, ROWS:] - delta) * SCALE).astype(BF16)
        kv_part[0, :, here] = jnp.dot(
            jnp.concatenate([dscore[:ROWS], ahead], axis=1),
            jnp.concatenate([query, q_next[:, here]], axis=0),
            preferred_element_type=F32,
        ).astype(BF16)
        send(7, u)
        kv_sum[0, :, here] = jnp.dot(dscore[ROWS:], query, preferred_element_type=F32)
        q_sum[:, here] = lax.dot_general(
            dscore, jnp.concatenate([key_near, kv_ref[0, :, here]], axis=0), FIRST,
            preferred_element_type=F32,
        )

    def finish(u):
        here = head(u)
        receive(5, u)
        gq_ref[:, here] = (q_got[:, here].astype(F32) + q_sum[:, here]).astype(BF16)
        receive(6, u)
        receive(7, u)
        gkv_ref[:, :, here] = (kv_got[:, :, here].astype(F32) + kv_sum[:, :, here]).astype(BF16)

    def early(begin, end):
        pl.loop(begin, end)(score)

    for c in range(LEAD // 2, COUNT):
        kv_load(c).wait()
    early(0, 2)
    for r in range(4):
        if r > 0:
            tags_to(4 - r).wait_recv()
            grad_to(4 - r).wait_recv()
            text = down(tagb[r - 1]) == 1.0
        else:
            text = down(tags_ref[...]) == 1.0
        for j in range(4):
            if r > 0:
                block = gyb[r - 1, :, j * 128 : (j + 1) * 128]
            else:
                block = gy_ref[:, place(x * 4 + j)]
            block = block.astype(F32)
            rows = slice(r * ROWS, (r + 1) * ROWS)
            gm[rows, j * 128 : (j + 1) * 128] = jnp.where(text, block, 0.0).astype(BF16)
            gm[rows, PART + j * 128 : PART + (j + 1) * 128] = jnp.where(text, 0.0, block).astype(BF16)

    relay(0)
    project(0)
    early(2, 4)
    relay(1)
    project(1)
    early(4, EARLY)
    relay(2)

    @pl.loop(0, (HEADS + HOME + 1) // 2)
    def _(j):
        for b in range(2):
            u = 2 * j + b
            pl.when(u < HEADS)(lambda: collect(u))
            pl.when(u + EARLY < HEADS)(lambda: score(u + EARLY))
            pl.when(jnp.logical_and(u >= NEXT, u < HEADS + NEXT))(lambda: weigh(u - NEXT))
            pl.when(jnp.logical_and(u >= BACK, u < HEADS + BACK))(lambda: grads(u - BACK))
            if b == 0:
                pl.when(j + 2 < COUNT)(lambda: project(j + 2))
            else:
                pl.when(j + 3 < COUNT)(lambda: relay(j + 3))
            pl.when(jnp.logical_and(u >= HOME, u < HEADS + HOME))(lambda: finish(u - HOME))

    for o in range(1, 4):
        tags_to(o).wait_send()
        grad_to(o).wait_send()

    whole = wg.at[:, :, place(slot)]
    for kind in range(4):
        done = remote(whole, whole, s_w.at[kind], r_w.at[0, 0], partner)
        if kind < 2:
            pl.when(spreads)(done.wait_send)
        else:
            done.wait_send()
    for kind, (src, dst, to) in enumerate(moves):
        done = remote(src, dst, s_kv.at[kind], r_kv.at[0, 0], to)
        pl.when(has_after if forward[kind] else has_before)(done.wait_send)
    for o in range(1, 4):
        remote(psend.at[o - 1], precv.at[3 - o], s_p.at[o - 1], r_p.at[0, 0], across[o]).wait_send()


def shards(query, key_value, grad_y, tags, segments, out_weight):
    vmem = pl.BlockSpec(memory_space=pltpu.VMEM)
    dma = pltpu.SemaphoreType.DMA
    held = [
        pltpu.with_memory_space_constraint(array, pltpu.HBM)
        for array in (query[0], key_value[:, 0], grad_y[0], tags, segments, out_weight)
    ]
    pair = (2, ROWS, WIDTH)
    grad_q, grad_kv = pl.pallas_call(
        kernel,
        out_shape=(
            jax.ShapeDtypeStruct((ROWS, WIDTH), BF16),
            jax.ShapeDtypeStruct(pair, BF16),
        ),
        in_specs=[pl.BlockSpec(memory_space=pltpu.HBM)] * 6,
        out_specs=(vmem, vmem),
        scratch_shapes=[
            pltpu.VMEM((ROWS, WIDTH), BF16),
            pltpu.VMEM(pair, BF16),
            pltpu.VMEM((ROWS, WIDTH), BF16),
            pltpu.VMEM((1, ROWS), jnp.int32),
            pltpu.VMEM((1, WIDTH), jnp.int32),
            pltpu.VMEM((2, WIDTH, PART), BF16),
            pltpu.VMEM((3, ROWS, PART), BF16),
            pltpu.VMEM((3, 1, ROWS), jnp.int32),
            pltpu.VMEM((4 * ROWS, 2 * PART), BF16),
            pltpu.VMEM((3, ROWS, WIDTH), BF16),
            pltpu.VMEM((3, ROWS, WIDTH), BF16),
            pltpu.VMEM((ROWS, WIDTH), F32),
            pltpu.VMEM((3 * ROWS, ROWS), F32),
            pltpu.VMEM(pair, BF16),
            pltpu.VMEM((ROWS, WIDTH), BF16),
            pltpu.VMEM((ROWS, WIDTH), BF16),
            pltpu.VMEM((ROWS, WIDTH), BF16),
            pltpu.VMEM((HEADS, 3 * ROWS, ROWS), F32),
            pltpu.VMEM((HEADS, 3 * ROWS, ROWS), F32),
            *[pltpu.VMEM((HEADS, 2, ROWS), F32)] * 4,
            *[pltpu.VMEM((HEADS, 1, ROWS), F32)] * 4,
            pltpu.VMEM((ROWS, WIDTH), BF16),
            pltpu.VMEM((ROWS, WIDTH), BF16),
            pltpu.VMEM((ROWS, WIDTH), F32),
            pltpu.VMEM(pair, BF16),
            pltpu.VMEM(pair, BF16),
            pltpu.VMEM(pair, F32),
            dma((5,)), dma((COUNT,)),
            dma((3,)), dma((3,)), dma((3,)), dma((3,)),
            dma((4,)), dma((3, COUNT)),
            dma((3,)), dma((3, HEADS)),
            dma((10,)), dma((10, HEADS)),
        ],
        compiler_params=pltpu.CompilerParams(
            collective_id=1, has_side_effects=True, vmem_limit_bytes=48 << 20
        ),
        name="mixed_backward",
    )(*held)
    return grad_q[None], grad_kv[:, None]


def solution(mesh):
    return jax.shard_map(
        shards,
        mesh=mesh,
        in_specs=(
            P("dp", "seq", None),
            P(None, "dp", "seq", None),
            P("dp", "seq", None),
            P("dp", "seq"),
            P("dp", None),
            P(None, None, "dp"),
        ),
        out_specs=(P("dp", "seq", None), P(None, "dp", "seq", None)),
        check_vma=False,
    )
```

```python
import jax
import jax.numpy as jnp
from jax import lax
from jax.experimental import pallas as pl
from jax.experimental.pallas import tpu as pltpu
from jax.sharding import PartitionSpec as P

HEAD_DIM = 128
ROWS = 128
WIDTH = 2048
PART = 512
CHUNK = 256
COUNT = WIDTH // CHUNK
HEADS = WIDTH // HEAD_DIM
LEAD = 8
EARLY = 4
NEXT = 3
BACK = 7
HOME = 11
SCALE = HEAD_DIM ** -0.5
NEG = -1e30
F32 = jnp.float32
BF16 = jnp.bfloat16
MESH = pl.DeviceIdType.MESH
LAST = (((1,), (1,)), ((), ()))
FIRST = (((0,), (0,)), ((), ()))


def down(row):
    return jnp.broadcast_to(row.astype(F32), (ROWS, ROWS)).T


def kernel(
    q_in, kv_in, gy_in, tags_in, seg_in, w_in, gq_ref, gkv_ref,
    q_ref, kv_ref, gy_ref, tags_ref, seg_ref, wg, gyb, tagb, gm, psend, precv, pown, bias,
    near, q_next, grad_own, grad_next, raised, dprob, up_own, down_own, up_got, down_got,
    up_delta, down_delta, up_delta_got, down_delta_got, q_part, q_got, q_sum, kv_part, kv_got, kv_sum,
    in_sem, kv_sem, s_gy, r_gy, s_tag, r_tag, s_w, r_w, s_p, r_p, s_kv, r_kv,
):
    dp, seq = lax.axis_index("dp"), lax.axis_index("seq")
    x, slot, core = lax.div(dp, 4), lax.rem(dp, 4), lax.rem(dp, 2)
    y_lo = lax.div(slot, 2)
    other = lax.rem(slot + 2, 4)
    after, before = (dp, lax.rem(seq + 1, 16)), (dp, lax.rem(seq + 15, 16))
    has_after, has_before = seq < 15, seq > 0
    spreads = lax.div(seq, 8) != lax.div(lax.rem(seq, 8), 4)
    beside = dp + 2 - 4 * y_lo
    above = (beside, lax.rem(seq + 8 * y_lo, 16))
    below = (beside, lax.rem(seq + 8 - 8 * y_lo, 16))
    partner = (dp + 1 - 2 * core, seq)
    across = [None] + [(lax.rem(dp + 4 * o, 16), seq) for o in range(1, 4)]

    def cols(c):
        return pl.ds(pl.multiple_of(c * CHUNK, CHUNK), CHUNK)

    def place(number):
        return pl.ds(pl.multiple_of(number * 128, 128), 128)

    def head(u):
        return pl.ds(pl.multiple_of(u * HEAD_DIM, HEAD_DIM), HEAD_DIM)

    def kv_load(c):
        return pltpu.make_async_copy(kv_in.at[:, :, cols(c)], kv_ref.at[:, :, cols(c)], kv_sem.at[c])

    load_tags = pltpu.make_async_copy(tags_in, tags_ref, in_sem.at[0])
    load_gy = pltpu.make_async_copy(gy_in, gy_ref, in_sem.at[1])
    load_w = pltpu.make_async_copy(w_in, wg.at[:, :, place(slot)], in_sem.at[2])
    load_seg = pltpu.make_async_copy(seg_in, seg_ref, in_sem.at[3])
    load_q = pltpu.make_async_copy(q_in, q_ref, in_sem.at[4])
    load_tags.start()
    load_gy.start()
    for c in range(2):
        kv_load(c).start()
    load_w.start()
    load_seg.start()
    load_q.start()
    for c in range(2, COUNT):
        kv_load(c).start()
    barrier = pltpu.get_barrier_semaphore()
    for peer in (after, before, above, below, partner, *across[1:]):
        pl.semaphore_signal(barrier, inc=1, device_id=peer, device_id_type=MESH)
    pl.semaphore_wait(barrier, 8)

    def remote(src, dst, send, recv, to):
        return pltpu.make_async_remote_copy(
            src_ref=src, dst_ref=dst, send_sem=send, recv_sem=recv,
            device_id=to, device_id_type=MESH,
        )

    def tags_to(o):
        return remote(tags_ref, tagb.at[3 - o], s_tag.at[o - 1], r_tag.at[3 - o], across[o])

    def grad_to(o):
        part = pl.ds(pl.multiple_of(lax.rem(x + o, 4) * PART, PART), PART)
        return remote(gy_ref.at[:, part], gyb.at[3 - o], s_gy.at[o - 1], r_gy.at[3 - o], across[o])

    def weight_to(kind, c):
        piece = wg.at[:, cols(c), place(other if kind == 3 else slot)]
        to = (above, below, partner, partner)[kind]
        return remote(piece, piece, s_w.at[kind], r_w.at[max(kind - 1, 0), c], to)

    def partial_to(o, u):
        return remote(
            psend.at[o - 1, :, head(u)], precv.at[3 - o, :, head(u)],
            s_p.at[o - 1], r_p.at[3 - o, u], across[o],
        )

    moves = (
        (kv_ref, near, after),
        (q_ref, q_next, before),
        (grad_own, grad_next, before),
        (up_own, up_got, before),
        (down_own, down_got, after),
        (q_part, q_got, after),
        (kv_part.at[1], kv_got.at[1], before),
        (kv_part.at[0], kv_got.at[0], before),
        (up_delta, up_delta_got, before),
        (down_delta, down_delta_got, after),
    )
    forward = (True, False, False, False, True, True, False, False, False, True)

    def move(kind, u):
        src, dst, to = moves[kind]
        if kind in (3, 4, 8, 9):
            src, dst = src.at[u], dst.at[u]
        elif kind == 0:
            src, dst = src.at[:, :, head(u)], dst.at[:, :, head(u)]
        else:
            src, dst = src.at[:, head(u)], dst.at[:, head(u)]
        return remote(src, dst, s_kv.at[kind], r_kv.at[kind, u], to)

    def send(kind, c):
        pl.when(has_after if forward[kind] else has_before)(lambda: move(kind, c).start())

    def receive(kind, c):
        pl.when(has_before if forward[kind] else has_after)(lambda: move(kind, c).wait_recv())

    load_tags.wait()
    load_gy.wait()
    for o in (2, 1, 3):
        tags_to(o).start()
        grad_to(o).start()
    for c in range(LEAD // 2):
        kv_load(c).wait()
        send(0, 2 * c)
        send(0, 2 * c + 1)
    load_q.wait()

    @pl.loop(0, HEADS)
    def _(u):
        send(1, u)

    load_w.wait()

    @pl.loop(0, COUNT)
    def _(c):
        @pl.when(spreads)
        def _():
            weight_to(0, c).start()
            weight_to(1, c).start()

        weight_to(2, c).start()

    first_rows = lax.broadcasted_iota(jnp.int32, (HEADS, 2, ROWS), 1)

    @pl.when(jnp.logical_not(has_before))
    def _():
        near[...] = jnp.zeros_like(near)
        q_got[...] = jnp.zeros_like(q_got)
        down_got[...] = jnp.where(first_rows == 0, NEG, 0.0).astype(F32)
        down_delta_got[...] = jnp.zeros_like(down_delta_got)

    @pl.when(jnp.logical_not(has_after))
    def _():
        q_next[...] = jnp.zeros_like(q_next)
        grad_next[...] = jnp.zeros_like(grad_next)
        kv_got[...] = jnp.zeros_like(kv_got)
        up_got[...] = jnp.ones_like(up_got)
        up_delta_got[...] = jnp.zeros_like(up_delta_got)

    load_seg.wait()
    behind, ahead = jnp.maximum(seq - 1, 0), jnp.minimum(seq + 1, 15)
    near_valid = jnp.where(has_before, 0.0, NEG).astype(F32)
    next_valid = jnp.where(has_after, near_valid, NEG).astype(F32)
    for part, (key_block, query_block) in enumerate(((behind, ahead), (behind, seq), (seq, seq))):
        query_row = seg_ref[:, place(query_block)].astype(F32)
        same = down(seg_ref[:, place(key_block)]) == jnp.broadcast_to(query_row, (ROWS, ROWS))
        if part == 2:
            key = lax.broadcasted_iota(jnp.int32, (ROWS, ROWS), 0)
            query = lax.broadcasted_iota(jnp.int32, (ROWS, ROWS), 1)
            block = jnp.where(jnp.logical_and(same, key <= query), 0.0, NEG)
        else:
            block = jnp.where(same, (next_valid, near_valid)[part], NEG)
        bias[part * ROWS : (part + 1) * ROWS, :] = block

    def relay(c):
        weight_to(0, c).wait_recv()
        weight_to(3, c).start()

    def project(c):
        weight_to(2, c).wait_recv()
        weight_to(3, c).wait_recv()
        total = lax.dot_general(
            gm[:, :PART], wg[1, cols(c), :], LAST, preferred_element_type=F32
        ) + lax.dot_general(gm[:, PART:], wg[0, cols(c), :], LAST, preferred_element_type=F32)
        pown[:, cols(c)] = total[:ROWS]
        for o in (2, 1, 3):
            psend[o - 1, :, cols(c)] = total[o * ROWS : (o + 1) * ROWS].astype(BF16)
        for h in range(2):
            for o in (2, 1, 3):
                partial_to(o, 2 * c + h).start()

    def collect(u):
        for o in range(1, 4):
            partial_to(o, u).wait_recv()
        grad = pown[:, head(u)]
        for r in range(3):
            grad = grad + precv[r, :, head(u)].astype(F32)
        grad_own[:, head(u)] = grad.astype(BF16)
        send(2, u)

    row = lax.broadcasted_iota(jnp.int32, (2, ROWS), 0)

    def partial_rows(keys, query, mask):
        scores = lax.dot_general(keys, query, LAST, preferred_element_type=F32) * SCALE + mask
        top = jnp.max(scores, axis=0, keepdims=True)
        power = jnp.exp(scores - top)
        return power, jnp.where(row == 0, top, jnp.sum(power, axis=0, keepdims=True))

    def score(u):
        here = head(u)
        receive(0, u)
        pl.when(u + LEAD < HEADS)(lambda: send(0, u + LEAD))
        receive(1, u)
        raised[u, :ROWS], down_own[u] = partial_rows(near[0, :, here], q_next[:, here], bias[:ROWS])
        send(4, u)
        keys = jnp.concatenate([near[0, :, here], kv_ref[0, :, here]], axis=0)
        raised[u, ROWS:], up_own[u] = partial_rows(keys, q_ref[:, here], bias[ROWS:])
        send(3, u)

    def merge(mine, got, u):
        top, total = (mine[u, r : r + 1, :] for r in range(2))
        top_got, total_got = (got[u, r : r + 1, :] for r in range(2))
        both = jnp.maximum(top, top_got)
        weight, weight_got = jnp.exp(top - both), jnp.exp(top_got - both)
        return weight / (total * weight + total_got * weight_got)

    def weigh(u):
        here = head(u)
        for kind in (2, 3, 4):
            receive(kind, u)
        grad, grad_ahead = grad_own[:, here], grad_next[:, here]
        value_near, value_own = near[1, :, here], kv_ref[1, :, here]
        ahead_grads = lax.dot_general(value_near, grad_ahead, LAST, preferred_element_type=F32)
        ahead_probs = raised[u, :ROWS] * merge(down_own, up_got, u)
        total = jnp.sum(ahead_probs * ahead_grads, axis=0, keepdims=True)
        down_delta[u] = total
        send(9, u)
        values = jnp.concatenate([value_near, value_own], axis=0)
        grads = lax.dot_general(values, grad, LAST, preferred_element_type=F32)
        probs = raised[u, ROWS:] * merge(up_own, down_got, u)
        up_delta[u] = jnp.sum(probs * grads, axis=0, keepdims=True)
        send(8, u)
        raised[u, :ROWS], raised[u, ROWS:] = ahead_probs, probs
        dprob[u, :ROWS], dprob[u, ROWS:] = ahead_grads, grads
        probs = probs.astype(BF16)
        kv_part[1, :, here] = jnp.dot(
            jnp.concatenate([probs[:ROWS], ahead_probs.astype(BF16)], axis=1),
            jnp.concatenate([grad, grad_ahead], axis=0),
            preferred_element_type=F32,
        ).astype(BF16)
        send(6, u)
        kv_sum[1, :, here] = jnp.dot(probs[ROWS:], grad, preferred_element_type=F32)

    def grads(u):
        here = head(u)
        receive(8, u)
        receive(9, u)
        delta = down_delta[u] + up_delta_got[u]
        ahead = (raised[u, :ROWS] * (dprob[u, :ROWS] - delta) * SCALE).astype(BF16)
        query, key_near = q_ref[:, here], near[0, :, here]
        q_part[:, here] = lax.dot_general(
            ahead, key_near, FIRST, preferred_element_type=F32
        ).astype(BF16)
        send(5, u)
        delta = up_delta[u] + down_delta_got[u]
        dscore = (raised[u, ROWS:] * (dprob[u, ROWS:] - delta) * SCALE).astype(BF16)
        kv_part[0, :, here] = jnp.dot(
            jnp.concatenate([dscore[:ROWS], ahead], axis=1),
            jnp.concatenate([query, q_next[:, here]], axis=0),
            preferred_element_type=F32,
        ).astype(BF16)
        send(7, u)
        kv_sum[0, :, here] = jnp.dot(dscore[ROWS:], query, preferred_element_type=F32)
        q_sum[:, here] = lax.dot_general(
            dscore, jnp.concatenate([key_near, kv_ref[0, :, here]], axis=0), FIRST,
            preferred_element_type=F32,
        )

    def finish(u):
        here = head(u)
        receive(5, u)
        gq_ref[:, here] = (q_got[:, here].astype(F32) + q_sum[:, here]).astype(BF16)
        receive(6, u)
        receive(7, u)
        gkv_ref[:, :, here] = (kv_got[:, :, here].astype(F32) + kv_sum[:, :, here]).astype(BF16)

    def early(begin, end):
        pl.loop(begin, end)(score)

    for c in range(LEAD // 2, COUNT):
        kv_load(c).wait()
    for r in range(4):
        if r > 0:
            tags_to(4 - r).wait_recv()
            grad_to(4 - r).wait_recv()
            text = down(tagb[r - 1]) == 1.0
        else:
            text = down(tags_ref[...]) == 1.0
        for j in range(4):
            if r > 0:
                block = gyb[r - 1, :, j * 128 : (j + 1) * 128]
            else:
                block = gy_ref[:, place(x * 4 + j)]
            block = block.astype(F32)
            rows = slice(r * ROWS, (r + 1) * ROWS)
            gm[rows, j * 128 : (j + 1) * 128] = jnp.where(text, block, 0.0).astype(BF16)
            gm[rows, PART + j * 128 : PART + (j + 1) * 128] = jnp.where(text, 0.0, block).astype(BF16)

    relay(0)
    project(0)
    early(0, 3)
    relay(1)
    project(1)
    early(3, EARLY)

    @pl.loop(0, (HEADS + HOME + 1) // 2)
    def _(j):
        for b in range(2):
            u = 2 * j + b
            pl.when(u < HEADS)(lambda: collect(u))
            pl.when(u + EARLY < HEADS)(lambda: score(u + EARLY))
            pl.when(jnp.logical_and(u >= NEXT, u < HEADS + NEXT))(lambda: weigh(u - NEXT))
            pl.when(jnp.logical_and(u >= BACK, u < HEADS + BACK))(lambda: grads(u - BACK))
            if b == 0:
                pl.when(j == 0)(lambda: relay(2))
                pl.when(j + 2 < COUNT)(lambda: project(j + 2))
            else:
                pl.when(j + 3 < COUNT)(lambda: relay(j + 3))
            pl.when(jnp.logical_and(u >= HOME, u < HEADS + HOME))(lambda: finish(u - HOME))

    for o in range(1, 4):
        tags_to(o).wait_send()
        grad_to(o).wait_send()

    whole = wg.at[:, :, place(slot)]
    for kind in range(4):
        done = remote(whole, whole, s_w.at[kind], r_w.at[0, 0], partner)
        if kind < 2:
            pl.when(spreads)(done.wait_send)
        else:
            done.wait_send()
    for kind, (src, dst, to) in enumerate(moves):
        done = remote(src, dst, s_kv.at[kind], r_kv.at[0, 0], to)
        pl.when(has_after if forward[kind] else has_before)(done.wait_send)
    for o in range(1, 4):
        remote(psend.at[o - 1], precv.at[3 - o], s_p.at[o - 1], r_p.at[0, 0], across[o]).wait_send()


def shards(query, key_value, grad_y, tags, segments, out_weight):
    vmem = pl.BlockSpec(memory_space=pltpu.VMEM)
    dma = pltpu.SemaphoreType.DMA
    held = [
        pltpu.with_memory_space_constraint(array, pltpu.HBM)
        for array in (query[0], key_value[:, 0], grad_y[0], tags, segments, out_weight)
    ]
    pair = (2, ROWS, WIDTH)
    grad_q, grad_kv = pl.pallas_call(
        kernel,
        out_shape=(
            jax.ShapeDtypeStruct((ROWS, WIDTH), BF16),
            jax.ShapeDtypeStruct(pair, BF16),
        ),
        in_specs=[pl.BlockSpec(memory_space=pltpu.HBM)] * 6,
        out_specs=(vmem, vmem),
        scratch_shapes=[
            pltpu.VMEM((ROWS, WIDTH), BF16),
            pltpu.VMEM(pair, BF16),
            pltpu.VMEM((ROWS, WIDTH), BF16),
            pltpu.VMEM((1, ROWS), jnp.int32),
            pltpu.VMEM((1, WIDTH), jnp.int32),
            pltpu.VMEM((2, WIDTH, PART), BF16),
            pltpu.VMEM((3, ROWS, PART), BF16),
            pltpu.VMEM((3, 1, ROWS), jnp.int32),
            pltpu.VMEM((4 * ROWS, 2 * PART), BF16),
            pltpu.VMEM((3, ROWS, WIDTH), BF16),
            pltpu.VMEM((3, ROWS, WIDTH), BF16),
            pltpu.VMEM((ROWS, WIDTH), F32),
            pltpu.VMEM((3 * ROWS, ROWS), F32),
            pltpu.VMEM(pair, BF16),
            pltpu.VMEM((ROWS, WIDTH), BF16),
            pltpu.VMEM((ROWS, WIDTH), BF16),
            pltpu.VMEM((ROWS, WIDTH), BF16),
            pltpu.VMEM((HEADS, 3 * ROWS, ROWS), F32),
            pltpu.VMEM((HEADS, 3 * ROWS, ROWS), F32),
            *[pltpu.VMEM((HEADS, 2, ROWS), F32)] * 4,
            *[pltpu.VMEM((HEADS, 1, ROWS), F32)] * 4,
            pltpu.VMEM((ROWS, WIDTH), BF16),
            pltpu.VMEM((ROWS, WIDTH), BF16),
            pltpu.VMEM((ROWS, WIDTH), F32),
            pltpu.VMEM(pair, BF16),
            pltpu.VMEM(pair, BF16),
            pltpu.VMEM(pair, F32),
            dma((5,)), dma((COUNT,)),
            dma((3,)), dma((3,)), dma((3,)), dma((3,)),
            dma((4,)), dma((3, COUNT)),
            dma((3,)), dma((3, HEADS)),
            dma((10,)), dma((10, HEADS)),
        ],
        compiler_params=pltpu.CompilerParams(
            collective_id=1, has_side_effects=True, vmem_limit_bytes=48 << 20
        ),
        name="mixed_backward",
    )(*held)
    return grad_q[None], grad_kv[:, None]


def solution(mesh):
    return jax.shard_map(
        shards,
        mesh=mesh,
        in_specs=(
            P("dp", "seq", None),
            P(None, "dp", "seq", None),
            P("dp", "seq", None),
            P("dp", "seq"),
            P("dp", None),
            P(None, None, "dp"),
        ),
        out_specs=(P("dp", "seq", None), P(None, "dp", "seq", None)),
        check_vma=False,
    )
```
